256 devices in a mesh: expert: 32 (over z_hi, y, core), dp: 8 (over z_lo, x).
Axes of the slice: x: 4, y: 4, z: 8 (z_hi: 4, z_lo: 2; z = z_hi * 2 + z_lo), core: 2. Of those that a mesh axis runs over, the one named last changes fastest.
Arguments:
- tokens: bfloat16 [32768, 4096], P(('expert', 'dp')), may hold values from -6 to 6
- route: int32 [32768, 2], P(('expert', 'dp')), may hold values from 0 to 63, all different within a row; in each aligned block of 128 rows (0 to 127, 128 to 255, ...) at most 12 rows name the same one
- gate_output_gradient: bfloat16 [32768, 2, 1536], P(('expert', 'dp')), may hold values from -0.4375 to 0.4375
- frozen_gate_weight: bfloat16 [64, 4096, 1536], P('expert', 'dp'), may hold values from -0.09375 to 0.09375
- adapter_first: bfloat16 [64, 4096, 16], P('expert'), may hold values from -0.09375 to 0.09375
- adapter_second: bfloat16 [64, 16, 1536], P('expert'), may hold values from -0.15625 to 0.15625
Outputs:
- grad_a: float32 [64, 4096, 16], P('expert')
- grad_b: float32 [64, 16, 1536], P('expert')
The draws below stay inside these ranges and needn't reach their ends.
Inputs may be any that keep to these rules, and one draw needn't show every extreme that they name: `route`: each row names 2 different experts. Within each device's aligned block of 128 rows no expert is named more than 12 times.
All inputs are finite; a program needn't handle non-finite values.
Results may differ from the reference program's by a relative error of at most 0.0043.
Values may be sent and summed in bfloat16 or wider, within the bound.
No kernel may reach another device: no remote copies, remote signals or barrier semaphores. Data moves between devices by JAX's collectives and lax.ppermute only.
A program may use at most 128 MiB of HBM per device.

```python
import math
import jax
import jax.numpy as jnp
import numpy as np
from jax import lax

MODEL_WIDTH = 4096
GATE_HIDDEN = 1536
ADAPTER_RANK = 16
TOP = 2
TOK_DEV = 128
EXPERT_TOTAL = 64
CAP = 12
TOKENS = 32768


def levels(own_key, shape, pieces, low, high):
    gain, own = 1.0, jax.random.fold_in(own_key, 6)
    for dim, parts in pieces:
        heights = jnp.exp(jax.random.uniform(jax.random.fold_in(own, dim), (parts,), jnp.float32, low / len(pieces), high / len(pieces)))
        gain = gain * jnp.repeat(heights, shape[dim] // parts).reshape([-1 if axis == dim else 1 for axis in range(len(shape))])
    return gain


def assign_block(stream_key, own, number, rows, amount, top, bound, lean):
    order = jax.random.permutation(stream_key, amount)
    heavy_load, common = load_shares(amount, rows * top, bound, lean, True), load_shares(amount, rows * top, bound, lean, False)
    places = jnp.arange(amount)

    def named(sizes, rotation):
        used = int((sizes > 0).sum())
        fixed = max(1, used // 4)
        shifted = fixed + (places - fixed + rotation * (used - fixed)) % max(1, amount - fixed)
        return jnp.zeros((amount,), jnp.int32).at[order[jnp.where(places < fixed, places, shifted)]].set(jnp.asarray(sizes, jnp.int32))

    sizes = jnp.where(number % 4 == 0, named(heavy_load, number // 4), named(common, number - number // 4 - 1))
    mixed = jax.random.permutation(jax.random.fold_in(own, 3), amount)
    source_of, receiver = mixed[0:amount // 2 * 2:2], mixed[1:amount // 2 * 2:2]
    slack = jnp.minimum(sizes[source_of] - 1, bound - sizes[receiver]) // 2
    slack = jnp.where((source_of == order[0]) | (receiver == order[0]) | (sizes[receiver] == 0), 0, jnp.maximum(slack, 0))
    shifted = jax.random.randint(jax.random.fold_in(own, 4), (amount // 2,), 0, 1 << 20) % (slack + 1)
    sizes = sizes.at[source_of].add(-shifted).at[receiver].add(shifted)
    items = jnp.searchsorted(jnp.cumsum(sizes), jnp.arange(rows * top), side="right").astype(jnp.int32)
    table = items.reshape(top, rows).T
    table = table[jax.random.permutation(jax.random.fold_in(own, 1), rows)]
    rotation = jax.random.randint(jax.random.fold_in(own, 2), (rows, 1), 0, top)
    return jnp.take_along_axis(table, (jnp.arange(top)[None, :] + rotation) % top, axis=1)


def load_shares(amount, total, limit, lean, full):
    portions = [(1 << 20) // math.isqrt(standing ** lean) + 1 for standing in range(1, amount + 1)]
    largest = limit if full else min(limit, max(-(-total // amount), total * portions[0] // sum(portions)))
    least = 1 if total - largest >= amount - 1 else 0
    given, rest = [largest] + [least] * (amount - 1), total - largest - least * (amount - 1)
    while rest > 0:
        movable = [i for i in range(1, amount) if given[i] < largest] or [i for i in range(1, amount) if given[i] < limit]
        pool, budget = sum([portions[i] for i in movable]), rest
        for i in movable:
            extra = min(limit - given[i], max(1, budget * portions[i] // pool), rest)
            given[i] = given[i] + extra
            rest = rest - extra
    return np.array(given)


def gaussian(rng, shape, deviation, most, split=(), kind=jnp.bfloat16):
    gain = levels(rng, shape, split, -0.22, 0.18) if split else 1.0
    drawn = jax.random.normal(rng, shape, jnp.float32) * deviation * gain
    return jnp.minimum(jnp.maximum(drawn, -most), most).astype(kind)


def setup_inputs(seed: int = 0) -> dict:
    splits = jax.random.split(jax.random.key(seed), 7)
    tokens = gaussian(splits[0], (TOKENS, MODEL_WIDTH), 1.0, 6.0, ((0, 256),))
    route_keys = jax.random.split(jax.random.fold_in(splits[1], 1), TOKENS // TOK_DEV)
    route_turns = jax.random.permutation(jax.random.fold_in(splits[1], 3), TOKENS // TOK_DEV)
    route = jax.vmap(lambda own, number: assign_block(jax.random.fold_in(splits[1], 2), own, number, TOK_DEV, EXPERT_TOTAL, TOP, CAP, 2))(route_keys, route_turns).reshape((TOKENS, TOP))
    gate_output_gradient = gaussian(splits[2], (TOKENS, TOP, GATE_HIDDEN), 0.03, 0.4375, ((0, 256),))
    frozen_gate_weight = gaussian(splits[3], (EXPERT_TOTAL, MODEL_WIDTH, GATE_HIDDEN), MODEL_WIDTH ** -0.5, 0.09375, ((0, 32), (1, 8)))
    adapter_first = gaussian(splits[4], (EXPERT_TOTAL, MODEL_WIDTH, ADAPTER_RANK), MODEL_WIDTH ** -0.5, 0.09375, ((0, 32),))
    adapter_second = gaussian(splits[5], (EXPERT_TOTAL, ADAPTER_RANK, GATE_HIDDEN), GATE_HIDDEN ** -0.5, 0.15625, ((0, 32),))
    return dict(tokens=tokens, route=route, gate_output_gradient=gate_output_gradient, frozen_gate_weight=frozen_gate_weight, adapter_first=adapter_first, adapter_second=adapter_second)


ADAPTER_SCALE = 2.0


def silu_slope(gate_preactivation):
    squash = jax.nn.sigmoid(gate_preactivation)
    return squash * (1.0 + gate_preactivation * (1.0 - squash))


def reference(tokens, route, gate_output_gradient, frozen_gate_weight, adapter_first, adapter_second):
    group_rows = 512
    slot_count = TOKENS * TOP
    flat_route = route.reshape(slot_count).astype(jnp.int32)
    order = jnp.argsort(flat_route, stable=True).astype(jnp.int32)
    labels = jnp.arange(EXPERT_TOTAL, dtype=jnp.int32)
    counts = jnp.sum((flat_route[:, None] == labels[None, :]).astype(jnp.int32), axis=0)
    starts = jnp.cumsum(counts) - counts
    padded = (counts + group_rows - 1) // group_rows * group_rows
    pad_starts = jnp.cumsum(padded) - padded
    block_count = slot_count // group_rows + EXPERT_TOTAL
    flat_grad = gate_output_gradient.reshape(slot_count, GATE_HIDDEN)

    def one_block(carry, block_index):
        down_gradient, up_gradient = carry
        first = block_index * group_rows
        expert_index = (jnp.sum((pad_starts <= first).astype(jnp.int32)) - 1).astype(jnp.int32)
        within = first + jnp.arange(group_rows, dtype=jnp.int32) - pad_starts[expert_index]
        valid = within < counts[expert_index]
        source = order[jnp.clip(starts[expert_index] + within, 0, slot_count - 1)]
        input_rows = tokens[source // TOP]
        rows_g = jnp.where(valid[:, None], flat_grad[source], jnp.zeros((), flat_grad.dtype))
        weight = frozen_gate_weight[expert_index]
        first_adapter_factor = adapter_first[expert_index]
        second_adapter_factor = adapter_second[expert_index]
        frozen_output = jnp.dot(input_rows, weight, preferred_element_type=jnp.float32)
        rank_reduced_output = jnp.dot(input_rows, first_adapter_factor, preferred_element_type=jnp.float32).astype(jnp.bfloat16)
        gate_preactivation = frozen_output + ADAPTER_SCALE * jnp.dot(rank_reduced_output, second_adapter_factor, preferred_element_type=jnp.float32)
        activation_slope = (rows_g.astype(jnp.float32) * silu_slope(gate_preactivation)).astype(jnp.bfloat16)
        up_portion = ADAPTER_SCALE * jnp.dot(rank_reduced_output.T, activation_slope, preferred_element_type=jnp.float32)
        rank_backward = jnp.dot(activation_slope, second_adapter_factor.T, preferred_element_type=jnp.float32).astype(jnp.bfloat16)
        down_portion = ADAPTER_SCALE * jnp.dot(input_rows.T, rank_backward, preferred_element_type=jnp.float32)
        down_gradient = down_gradient.at[expert_index].add(down_portion)
        up_gradient = up_gradient.at[expert_index].add(up_portion)
        return (down_gradient, up_gradient), None

    initial = (jnp.zeros((EXPERT_TOTAL, MODEL_WIDTH, ADAPTER_RANK), jnp.float32), jnp.zeros((EXPERT_TOTAL, ADAPTER_RANK, GATE_HIDDEN), jnp.float32))
    (grad_a, grad_b), _ = lax.scan(one_block, initial, jnp.arange(block_count, dtype=jnp.int32))
    return grad_a, grad_b
```

```python
import jax
import jax.numpy as jnp
from jax import lax
from jax.sharding import Mesh, PartitionSpec as P

ADAPTER_SCALE = 2.0
EXPERT_AXES = ("zh", "y", "c")
DP_AXES = ("zl", "x")
PLANE = ("zh", "y", "c", "zl")


def dot(a, b, dims=((1,), (0,))):
    return lax.dot_general(a, b, (dims, ((), ())), preferred_element_type=jnp.float32)


def silu_slope(gate_preactivation):
    squash = jax.nn.sigmoid(gate_preactivation)
    return squash * (1.0 + gate_preactivation * (1.0 - squash))


def slot_targets(route, cap):
    rows, top = route.shape
    flat = route.T.reshape(rows * top)
    before = jnp.arange(rows * top)[:, None] > jnp.arange(rows * top)[None, :]
    same = flat[:, None] == flat[None, :]
    ranks = jnp.sum((same & before).astype(jnp.int32), axis=1)
    return (flat * cap + ranks).reshape(top, rows)


def send_places(experts, cap, swap):
    p = jnp.arange(experts * 24, dtype=jnp.int32)
    e, piece, r = p // 24, p % 24 // 8, p % 8
    rank = jnp.where(piece < 2, r, 8 + r % 4)
    half = jnp.where(piece < 2, piece, r // 4)
    if swap:
        half = jnp.where(e % 2 == 1, 1 - half, half)
    return e * cap + rank, half


def local(tokens, route, gate_output_gradient, frozen_gate_weight, adapter_first, adapter_second):
    tok_rows, width = tokens.shape
    hidden = gate_output_gradient.shape[2]
    experts = 64
    cap = 12
    zl = lax.axis_index("zl")

    mine = lax.dynamic_index_in_dim(frozen_gate_weight, zl, 0, keepdims=False)
    other = lax.dynamic_index_in_dim(frozen_gate_weight, 1 - zl, 0, keepdims=False)
    weight_near = lax.all_gather(mine, "x", axis=0, tiled=True)
    got = lax.ppermute(other, "zl", [(0, 1), (1, 0)])
    weight_far = lax.all_gather(got, "x", axis=0, tiled=True)
    first = lax.dynamic_index_in_dim(adapter_first, zl, 0, keepdims=False)
    second = lax.dynamic_index_in_dim(adapter_second, zl, 0, keepdims=False)
    half_width = width // 2
    first = jnp.where(zl == 0, first, jnp.roll(first, half_width, axis=0))

    target = slot_targets(route, cap)
    place, half = send_places(experts, cap, True)
    match = (place[:, None] == target[0][None, :]) | (place[:, None] == target[1][None, :])
    pick = jnp.concatenate([match & (half == 0)[:, None], match & (half == 1)[:, None]], axis=1)
    stack = jnp.concatenate([tokens[:, :half_width], tokens[:, half_width:]], axis=0)
    send_x = dot(pick.astype(jnp.bfloat16), stack).astype(jnp.bfloat16)
    send_x = send_x.reshape(experts, 24, half_width)
    recv_x = lax.all_to_all(send_x, PLANE, split_axis=0, concat_axis=0, tiled=True)

    place, half = send_places(experts, cap, False)
    match = place[:, None] == target.reshape(1, 2 * tok_rows)
    pick = jnp.concatenate([match & (half == 0)[:, None], match & (half == 1)[:, None]], axis=1)
    half_hidden = hidden // 2
    parts = [
        gate_output_gradient[:, k, h * half_hidden : (h + 1) * half_hidden]
        for h in range(2)
        for k in range(2)
    ]
    send_g = dot(pick.astype(jnp.bfloat16), jnp.concatenate(parts, axis=0)).astype(jnp.bfloat16)
    send_g = send_g.reshape(experts, 24, half_hidden)
    recv_g = lax.all_to_all(send_g, PLANE, split_axis=0, concat_axis=0, tiled=True)

    row = jnp.arange(4 * experts)
    col = jnp.arange(8 * experts)
    same_source = (row // 4)[:, None] == (col // 8)[None, :]

    def gather_half(received, h):
        main = received[:, 8 * h : 8 * h + 8].reshape(8 * experts, -1)
        tail = received[:, 16:24].reshape(8 * experts, -1)
        pick = same_source & ((4 * h + row % 4)[:, None] == (col % 8)[None, :])
        tail = dot(pick.astype(jnp.bfloat16), tail).astype(jnp.bfloat16)
        return jnp.concatenate([main, tail], axis=0)

    x_near = gather_half(recv_x, 0)
    x_far = gather_half(recv_x, 1)
    low = (dot(x_near, first[:half_width]) + dot(x_far, first[half_width:])).astype(jnp.bfloat16)
    frozen = dot(x_near, weight_near) + dot(x_far, weight_far)
    preact = frozen + ADAPTER_SCALE * dot(low, second)
    rows_g = jnp.concatenate([gather_half(recv_g, 0), gather_half(recv_g, 1)], axis=1)
    slope = (rows_g.astype(jnp.float32) * silu_slope(preact)).astype(jnp.bfloat16)
    back = dot(slope, second, ((1,), (1,))).astype(jnp.bfloat16)
    grads = ADAPTER_SCALE * jnp.concatenate(
        [
            dot(back, x_near, ((0,), (0,))),
            dot(back, x_far, ((0,), (0,))),
            dot(low, slope, ((0,), (0,))),
        ],
        axis=1,
    )

    rank = grads.shape[0]
    chunk = grads.shape[1] // 4
    parts = grads.reshape(rank, 4, chunk).transpose(1, 0, 2)
    parts = lax.all_to_all(parts, "x", split_axis=0, concat_axis=0, tiled=True)
    total = jnp.sum(parts, axis=0).astype(jnp.bfloat16)
    total = jnp.broadcast_to(total[None], (8, rank, chunk))
    total = lax.all_to_all(total, DP_AXES, split_axis=0, concat_axis=0, tiled=True)
    total = total.reshape(2, 4, rank, chunk).transpose(0, 2, 1, 3).reshape(2, rank, 4 * chunk)
    near, far = total[:, :, :half_width], total[:, :, half_width:width]
    grad_a = jnp.stack(
        [
            jnp.concatenate([near[0], far[0]], axis=1),
            jnp.concatenate([far[1], near[1]], axis=1),
        ]
    )
    grad_a = grad_a.transpose(0, 2, 1).astype(jnp.float32)
    return grad_a, total[:, :, width:].astype(jnp.float32)


def solution(mesh):
    fine = Mesh(mesh.devices.reshape(4, 4, 2, 2, 4), EXPERT_AXES + DP_AXES)
    everyone = EXPERT_AXES + DP_AXES
    return jax.shard_map(
        local,
        mesh=fine,
        in_specs=(
            P(everyone, None),
            P(everyone, None),
            P(everyone, None, None),
            P(EXPERT_AXES, DP_AXES, None),
            P(EXPERT_AXES, None, None),
            P(EXPERT_AXES, None, None),
        ),
        out_specs=(P(EXPERT_AXES, None, None), P(EXPERT_AXES, None, None)),
        check_vma=False,
    )
```

```python
import jax
import jax.numpy as jnp
from jax import lax
from jax.sharding import Mesh, PartitionSpec as P

ADAPTER_SCALE = 2.0
EXPERT_AXES = ("zh", "y", "c")
DP_AXES = ("zl", "x")
PLANE = ("zh", "y", "c", "zl")


def dot(a, b, dims=((1,), (0,))):
    return lax.dot_general(a, b, (dims, ((), ())), preferred_element_type=jnp.float32)


def silu_slope(gate_preactivation):
    squash = jax.nn.sigmoid(gate_preactivation)
    return squash * (1.0 + gate_preactivation * (1.0 - squash))


def slot_targets(route, cap):
    rows, top = route.shape
    flat = route.T.reshape(rows * top)
    before = jnp.arange(rows * top)[:, None] > jnp.arange(rows * top)[None, :]
    same = flat[:, None] == flat[None, :]
    ranks = jnp.sum((same & before).astype(jnp.int32), axis=1)
    return (flat * cap + ranks).reshape(top, rows)


def send_places(experts, cap, swap):
    p = jnp.arange(experts * 24, dtype=jnp.int32)
    e, piece, r = p // 24, p % 24 // 8, p % 8
    rank = jnp.where(piece < 2, r, 8 + r % 4)
    half = jnp.where(piece < 2, piece, r // 4)
    if swap:
        half = jnp.where(e % 2 == 1, 1 - half, half)
    return e * cap + rank, half


RIGHT = [(i, (i + 1) % 4) for i in range(4)]
LEFT = [(i, (i - 1) % 4) for i in range(4)]


def first_hop(shard):
    return lax.ppermute(shard, "x", RIGHT), lax.ppermute(shard, "x", LEFT)


def second_hop(before, after):
    half = before.shape[0] // 2
    return lax.ppermute(before[:half], "x", RIGHT), lax.ppermute(after[half:], "x", LEFT)


def place_rows(buffer, shard, hop, opposite, x, base):
    rows = shard.shape[0]
    pieces = (
        (shard, x * rows),
        (hop[0], (x + 3) % 4 * rows),
        (hop[1], (x + 1) % 4 * rows),
        (opposite[0], (x + 2) % 4 * rows),
        (opposite[1], (x + 2) % 4 * rows + rows // 2),
    )
    for piece, start in pieces:
        buffer = lax.dynamic_update_slice(buffer, piece, (base + start, 0))
    return buffer


def local(tokens, route, gate_output_gradient, frozen_gate_weight, adapter_first, adapter_second):
    tok_rows, width = tokens.shape
    hidden = gate_output_gradient.shape[2]
    experts = 64
    cap = 12
    depth = 8
    zh, zl, x = lax.axis_index("zh"), lax.axis_index("zl"), lax.axis_index("x")
    half_width = width // 2

    lines = [
        lax.all_gather(tokens[:, h * half_width : (h + 1) * half_width], ("zh", "zl"), axis=0, tiled=True)
        for h in range(2)
    ]

    mine = lax.dynamic_index_in_dim(frozen_gate_weight, zl, 0, keepdims=False)
    other = lax.dynamic_index_in_dim(frozen_gate_weight, 1 - zl, 0, keepdims=False)
    got = lax.ppermute(other, "zl", [(0, 1), (1, 0)])
    near = first_hop(mine)
    line0, got, near = lax.optimization_barrier((lines[0], got, near))
    near_opposite = second_hop(*near)
    far = first_hop(got)
    line1, near_opposite, far = lax.optimization_barrier((lines[1], near_opposite, far))
    far_opposite = second_hop(*far)
    weight = jnp.zeros((width, hidden), jnp.bfloat16)
    weight = place_rows(weight, mine, near, near_opposite, x, zl * half_width)
    weight = place_rows(weight, got, far, far_opposite, x, (1 - zl) * half_width)
    first = lax.dynamic_index_in_dim(adapter_first, zl, 0, keepdims=False)
    second = lax.dynamic_index_in_dim(adapter_second, zl, 0, keepdims=False)

    target = slot_targets(route, cap)
    line_target = jnp.broadcast_to(target[None], (depth, 2, tok_rows))
    line_target = lax.all_to_all(line_target, ("zh", "zl"), split_axis=0, concat_axis=0, tiled=True)
    line_target = line_target.transpose(1, 0, 2).reshape(2, depth * tok_rows)
    row = jnp.arange(depth * depth * cap, dtype=jnp.int32)
    served = (zh * depth + row // (depth * cap)) * 2 + zl
    key = (served * cap + row % cap)[:, None]
    col = jnp.arange(depth * tok_rows, dtype=jnp.int32)
    same_block = (row // cap % depth)[:, None] == (col // tok_rows)[None, :]
    pick = same_block & ((line_target[0][None] == key) | (line_target[1][None] == key))
    pick = pick.astype(jnp.bfloat16)

    def spread(line):
        rows = dot(pick, line).astype(jnp.bfloat16).reshape(depth, depth * cap, half_width)
        rows = lax.all_to_all(rows, ("y", "c"), split_axis=0, concat_axis=0, tiled=True)
        return rows.reshape(depth * depth * cap, half_width)

    place, half = send_places(experts, cap, False)
    match = place[:, None] == target.reshape(1, 2 * tok_rows)
    pick_g = jnp.concatenate([match & (half == 0)[:, None], match & (half == 1)[:, None]], axis=1)
    half_hidden = hidden // 2
    parts = [
        gate_output_gradient[:, k, h * half_hidden : (h + 1) * half_hidden]
        for h in range(2)
        for k in range(2)
    ]
    send_g = dot(pick_g.astype(jnp.bfloat16), jnp.concatenate(parts, axis=0)).astype(jnp.bfloat16)
    send_g = send_g.reshape(experts, 24, half_hidden)

    x0 = spread(line0)
    send_g, line1 = lax.optimization_barrier((send_g, line1))
    x1 = spread(line1)
    recv_g = lax.all_to_all(send_g, PLANE, split_axis=0, concat_axis=0, tiled=True)
    recv_g = recv_g.reshape(experts * 24, half_hidden)

    block, rank = row // cap, row % cap
    source = block // 2 % 4 * 16 + block // 8 * 2 + block % 2
    q = jnp.arange(experts * 24, dtype=jnp.int32)

    def gather_half(h):
        at = source * 24 + jnp.where(rank < 8, 8 * h + rank, 16 + 4 * h + rank - 8)
        return dot((at[:, None] == q[None, :]).astype(jnp.bfloat16), recv_g)

    low = (dot(x0, first[:half_width]) + dot(x1, first[half_width:])).astype(jnp.bfloat16)
    frozen = dot(x0, weight[:half_width]) + dot(x1, weight[half_width:])
    preact = frozen + ADAPTER_SCALE * dot(low, second)
    rows_g = jnp.concatenate([gather_half(0), gather_half(1)], axis=1)
    slope = (rows_g * silu_slope(preact)).astype(jnp.bfloat16)
    back = dot(slope, second, ((1,), (1,))).astype(jnp.bfloat16)
    grads = ADAPTER_SCALE * jnp.concatenate(
        [
            dot(back, x0, ((0,), (0,))),
            dot(back, x1, ((0,), (0,))),
            dot(low, slope, ((0,), (0,))),
        ],
        axis=1,
    )

    rank = grads.shape[0]
    chunk = grads.shape[1] // 4
    parts = grads.reshape(rank, 4, chunk).transpose(1, 0, 2)
    parts = lax.all_to_all(parts, "x", split_axis=0, concat_axis=0, tiled=True)
    total = jnp.sum(parts, axis=0).astype(jnp.bfloat16)
    total = jnp.broadcast_to(total[None], (8, rank, chunk))
    total = lax.all_to_all(total, DP_AXES, split_axis=0, concat_axis=0, tiled=True)
    total = total.reshape(2, 4, rank, chunk).transpose(0, 2, 1, 3).reshape(2, rank, 4 * chunk)
    grad_a = total[:, :, :width].transpose(0, 2, 1).astype(jnp.float32)
    return grad_a, total[:, :, width:].astype(jnp.float32)


def solution(mesh):
    fine = Mesh(mesh.devices.reshape(4, 4, 2, 2, 4), EXPERT_AXES + DP_AXES)
    everyone = EXPERT_AXES + DP_AXES
    return jax.shard_map(
        local,
        mesh=fine,
        in_specs=(
            P(everyone, None),
            P(everyone, None),
            P(everyone, None, None),
            P(EXPERT_AXES, DP_AXES, None),
            P(EXPERT_AXES, None, None),
            P(EXPERT_AXES, None, None),
        ),
        out_specs=(P(EXPERT_AXES, None, None), P(EXPERT_AXES, None, None)),
        check_vma=False,
    )
```

```python
import jax
import jax.numpy as jnp
from jax import lax
from jax.experimental import pallas as pl
from jax.experimental.pallas import tpu as pltpu
from jax.sharding import Mesh, PartitionSpec as P

ADAPTER_SCALE = 2.0
EXPERT_AXES = ("zh", "y", "c")
DP_AXES = ("zl", "x")
PLANE = ("zh", "y", "c", "zl")


def dot(a, b, dims=((1,), (0,))):
    return lax.dot_general(a, b, (dims, ((), ())), preferred_element_type=jnp.float32)


def silu_slope(gate_preactivation):
    squash = jax.nn.sigmoid(gate_preactivation)
    return squash * (1.0 + gate_preactivation * (1.0 - squash))


def slot_targets(route, cap):
    rows, top = route.shape
    flat = route.T.reshape(rows * top)
    before = jnp.arange(rows * top)[:, None] > jnp.arange(rows * top)[None, :]
    same = flat[:, None] == flat[None, :]
    ranks = jnp.sum((same & before).astype(jnp.int32), axis=1)
    return (flat * cap + ranks).reshape(top, rows)


def send_places(experts, cap, swap):
    p = jnp.arange(experts * 24, dtype=jnp.int32)
    e, piece, r = p // 24, p % 24 // 8, p % 8
    rank = jnp.where(piece < 2, r, 8 + r % 4)
    half = jnp.where(piece < 2, piece, r // 4)
    if swap:
        half = jnp.where(e % 2 == 1, 1 - half, half)
    return e * cap + rank, half


RIGHT = [(i, (i + 1) % 4) for i in range(4)]
LEFT = [(i, (i - 1) % 4) for i in range(4)]


def first_hop(shard):
    return lax.ppermute(shard, "x", RIGHT), lax.ppermute(shard, "x", LEFT)


def second_hop(before, after):
    half = before.shape[0] // 2
    return lax.ppermute(before[:half], "x", RIGHT), lax.ppermute(after[half:], "x", LEFT)


def weight_products(where_ref, x_ref, pieces):
    x, zl = where_ref[0], where_ref[1]
    width = x_ref.shape[1] // 8
    total = None
    for n, piece in enumerate(pieces):
        line = zl if n < 4 else 1 - zl
        at = pl.multiple_of((line * 4 + (x + (0, 3, 1, 2)[n % 4]) % 4) * width, width)
        product = dot(x_ref[:, pl.ds(at, width)], piece[...])
        total = product if total is None else total + product
    return total


def half_kernel(where_ref, x_ref, first_ref, *refs):
    frozen_ref, low_ref = refs[8:]
    frozen_ref[...] = weight_products(where_ref, x_ref, refs[:8])
    low_ref[...] = dot(x_ref[...], first_ref[...], ((1,), (1,)))


def final_kernel(where_ref, xa_ref, xb_ref, g0_ref, g1_ref, frozen_ref, lowa_ref, first_ref, second_ref, *refs):
    out_ref, frozen_acc, slope_acc, sums = refs[8:]
    step = pl.program_id(0)
    low = (lowa_ref[...] + dot(xb_ref[...], first_ref[...], ((1,), (1,)))).astype(jnp.bfloat16)
    frozen_acc[...] = frozen_ref[...] + weight_products(where_ref, xb_ref, refs[:8])
    half = g0_ref.shape[1]
    for h, g_ref in enumerate((g0_ref, g1_ref)):
        cols = slice(h * half, (h + 1) * half)
        preact = frozen_acc[:, cols] + ADAPTER_SCALE * dot(low, second_ref[:, cols])
        slope = g_ref[...].astype(jnp.float32) * silu_slope(preact)
        slope_acc[:, cols] = slope.astype(jnp.bfloat16)
    back = dot(slope_acc[...], second_ref[...], ((1,), (1,))).astype(jnp.bfloat16)

    @pl.when(step == 0)
    def _():
        sums[...] = jnp.zeros_like(sums)

    width = xa_ref.shape[1] // 8
    for h, x_ref in enumerate((xa_ref, xb_ref)):
        part = dot(back, x_ref[...], ((0,), (0,)))
        for n in range(8):
            at = (2 * n + h) * width
            sums[:, at : at + width] += part[:, n * width : (n + 1) * width]
    sums[:, 16 * width :] += dot(low, slope_acc[...], ((0,), (0,)))

    @pl.when(step == pl.num_programs(0) - 1)
    def _():
        chunk = out_ref.shape[2]
        for n in range(4):
            out_ref[n] = ADAPTER_SCALE * sums[:, n * chunk : (n + 1) * chunk]


ROW_BLOCK = 256


def row_spec(array):
    return pl.BlockSpec((ROW_BLOCK, array.shape[1]), lambda i, w: (i, 0))


def whole_spec(array):
    return pl.BlockSpec(array.shape, lambda i, w: (0, 0))


def piece_specs(pieces, h):
    specs = []
    for piece in pieces:
        at = h if piece.shape[0] == 512 else 0
        specs.append(pl.BlockSpec((256, piece.shape[1]), lambda i, w, at=at: (at, 0)))
    return specs


def half_products(where, x, first, pieces, h):
    rows, hidden, rank = x.shape[0], pieces[0].shape[1], first.shape[0]
    return pl.pallas_call(
        half_kernel,
        grid_spec=pltpu.PrefetchScalarGridSpec(
            num_scalar_prefetch=1,
            grid=(rows // ROW_BLOCK,),
            in_specs=[row_spec(x), whole_spec(first)] + piece_specs(pieces, h),
            out_specs=[
                pl.BlockSpec((ROW_BLOCK, hidden), lambda i, w: (i, 0)),
                pl.BlockSpec((ROW_BLOCK, rank), lambda i, w: (i, 0)),
            ],
        ),
        out_shape=[
            jax.ShapeDtypeStruct((rows, hidden), jnp.float32),
            jax.ShapeDtypeStruct((rows, rank), jnp.float32),
        ],
        name="half_products",
    )(where, x, first, *pieces)


def gradients(where, xa, xb, g0, g1, frozen, low, first, second, pieces, h):
    rows, hidden, rank = xa.shape[0], pieces[0].shape[1], first.shape[0]
    total = 2 * xa.shape[1] + hidden
    by_row = [row_spec(v) for v in (xa, xb, g0, g1, frozen, low)]
    return pl.pallas_call(
        final_kernel,
        grid_spec=pltpu.PrefetchScalarGridSpec(
            num_scalar_prefetch=1,
            grid=(rows // ROW_BLOCK,),
            in_specs=by_row + [whole_spec(first), whole_spec(second)] + piece_specs(pieces, h),
            out_specs=pl.BlockSpec((4, rank, total // 4), lambda i, w: (0, 0, 0)),
            scratch_shapes=[
                pltpu.VMEM((ROW_BLOCK, hidden), jnp.float32),
                pltpu.VMEM((ROW_BLOCK, hidden), jnp.bfloat16),
                pltpu.VMEM((rank, total), jnp.float32),
            ],
        ),
        out_shape=jax.ShapeDtypeStruct((4, rank, total // 4), jnp.float32),
        name="gradients",
    )(where, xa, xb, g0, g1, frozen, low, first, second, *pieces)


def split_kernel(tokens_ref, *out_refs):
    for h, out_ref in enumerate(out_refs):
        for n in range(out_ref.shape[1] // 256):
            at = (2 * n + h) * 256
            out_ref[:, n * 256 : (n + 1) * 256] = tokens_ref[:, at : at + 256]


def split_columns(tokens):
    shape = jax.ShapeDtypeStruct((tokens.shape[0], tokens.shape[1] // 2), tokens.dtype)
    return pl.pallas_call(split_kernel, out_shape=[shape, shape], name="split_columns")(tokens)


def local(tokens, route, gate_output_gradient, frozen_gate_weight, adapter_first, adapter_second):
    tok_rows, width = tokens.shape
    hidden = gate_output_gradient.shape[2]
    experts = 64
    cap = 12
    depth = 8
    zh, zl, x = lax.axis_index("zh"), lax.axis_index("zl"), lax.axis_index("x")
    half_width = width // 2

    lines = [
        lax.all_gather(part, ("zh", "zl"), axis=0, tiled=True) for part in split_columns(tokens)
    ]

    target = slot_targets(route, cap)
    line_target = jnp.broadcast_to(target[None], (depth, 2, tok_rows))
    line_target = lax.all_to_all(line_target, ("zh", "zl"), split_axis=0, concat_axis=0, tiled=True)

    mine = lax.dynamic_index_in_dim(frozen_gate_weight, zl, 0, keepdims=False)
    other = lax.dynamic_index_in_dim(frozen_gate_weight, 1 - zl, 0, keepdims=False)
    near = first_hop(mine)
    other, line_target = lax.optimization_barrier((other, line_target))
    got = lax.ppermute(other, "zl", [(0, 1), (1, 0)])

    place, half = send_places(experts, cap, False)
    match = place[:, None] == target.reshape(1, 2 * tok_rows)
    pick_g = jnp.concatenate([match & (half == 0)[:, None], match & (half == 1)[:, None]], axis=1)
    half_hidden = hidden // 2
    parts = [
        gate_output_gradient[:, k, h * half_hidden : (h + 1) * half_hidden]
        for h in range(2)
        for k in range(2)
    ]
    send_g = dot(pick_g.astype(jnp.bfloat16), jnp.concatenate(parts, axis=0)).astype(jnp.bfloat16)
    send_g = send_g.reshape(experts, 24, half_hidden)
    send_g, line_target = lax.optimization_barrier((send_g, line_target))
    recv_g = lax.all_to_all(send_g, PLANE, split_axis=0, concat_axis=0, tiled=True)

    line_target = line_target.transpose(1, 0, 2).reshape(2, depth * tok_rows)
    row = jnp.arange(depth * depth * cap, dtype=jnp.int32)
    served = (zh * depth + row // (depth * cap)) * 2 + zl
    key = (served * cap + row % cap)[:, None]
    col = jnp.arange(depth * tok_rows, dtype=jnp.int32)
    same_block = (row // cap % depth)[:, None] == (col // tok_rows)[None, :]
    pick = same_block & ((line_target[0][None] == key) | (line_target[1][None] == key))
    pick = pick.astype(jnp.bfloat16)

    def packed(line):
        return dot(pick, line).astype(jnp.bfloat16).reshape(depth, depth * cap, half_width)

    def spread(rows):
        rows = lax.all_to_all(rows, ("y", "c"), split_axis=0, concat_axis=0, tiled=True)
        return rows.reshape(depth * depth * cap, half_width)

    line0, got, near = lax.optimization_barrier((lines[0], got, near))
    near_opposite = second_hop(*near)
    far = first_hop(got)
    send_0, recv_g = lax.optimization_barrier((packed(line0), recv_g))
    xa = spread(send_0)
    line1, near_opposite, far = lax.optimization_barrier((lines[1], near_opposite, far))
    far_opposite = second_hop(*far)
    xb = spread(packed(line1))

    recv_g = recv_g.reshape(experts * 24, half_hidden)
    block, rank = row // cap, row % cap
    source = block // 2 % 4 * 16 + block // 8 * 2 + block % 2
    q = jnp.arange(experts * 24, dtype=jnp.int32)

    def gather_half(h):
        at = source * 24 + jnp.where(rank < 8, 8 * h + rank, 16 + 4 * h + rank - 8)
        return dot((at[:, None] == q[None, :]).astype(jnp.bfloat16), recv_g).astype(jnp.bfloat16)

    first = lax.dynamic_index_in_dim(adapter_first, zl, 0, keepdims=False)
    second = lax.dynamic_index_in_dim(adapter_second, zl, 0, keepdims=False)
    first = first.T
    first_a, first_b = (
        jnp.concatenate([first[:, at : at + 256] for at in range(256 * h, width, 512)], axis=1)
        for h in range(2)
    )
    where = jnp.stack([x, zl]).astype(jnp.int32)
    pieces = [
        [mine, *near, near_opposite[h], got, *far, far_opposite[h]]
        for h in range(2)
    ]
    frozen, low = half_products(where, xa, first_a, pieces[0], 0)
    parts = gradients(
        where, xa, xb, gather_half(0), gather_half(1), frozen, low, first_b, second, pieces[1], 1
    )

    rank, chunk = parts.shape[1:]
    parts = lax.all_to_all(parts, "x", split_axis=0, concat_axis=0, tiled=True)
    total = jnp.sum(parts, axis=0).astype(jnp.bfloat16)
    total = jnp.broadcast_to(total[None], (8, rank, chunk))
    total = lax.all_to_all(total, DP_AXES, split_axis=0, concat_axis=0, tiled=True)
    total = total.reshape(2, 4, rank, chunk).transpose(0, 2, 1, 3).reshape(2, rank, 4 * chunk)
    grad_a = total[:, :, :width].transpose(0, 2, 1).astype(jnp.float32)
    return grad_a, total[:, :, width:].astype(jnp.float32)


def solution(mesh):
    fine = Mesh(mesh.devices.reshape(4, 4, 2, 2, 4), EXPERT_AXES + DP_AXES)
    everyone = EXPERT_AXES + DP_AXES
    return jax.shard_map(
        local,
        mesh=fine,
        in_specs=(
            P(everyone, None),
            P(everyone, None),
            P(everyone, None, None),
            P(EXPERT_AXES, DP_AXES, None),
            P(EXPERT_AXES, None, None),
            P(EXPERT_AXES, None, None),
        ),
        out_specs=(P(EXPERT_AXES, None, None), P(EXPERT_AXES, None, None)),
        check_vma=False,
    )
```

```python
import jax
import jax.numpy as jnp
from jax import lax
from jax.experimental import pallas as pl
from jax.experimental.pallas import tpu as pltpu
from jax.sharding import Mesh, PartitionSpec as P

ADAPTER_SCALE = 2.0
EXPERT_AXES = ("zh", "y", "c")
DP_AXES = ("zl", "x")
PLANE = ("zh", "y", "c", "zl")


def dot(a, b, dims=((1,), (0,))):
    return lax.dot_general(a, b, (dims, ((), ())), preferred_element_type=jnp.float32)


def silu_slope(gate_preactivation):
    squash = jax.nn.sigmoid(gate_preactivation)
    return squash * (1.0 + gate_preactivation * (1.0 - squash))


def slot_targets(route, cap):
    rows, top = route.shape
    flat = route.T.reshape(rows * top)
    before = jnp.arange(rows * top)[:, None] > jnp.arange(rows * top)[None, :]
    same = flat[:, None] == flat[None, :]
    ranks = jnp.sum((same & before).astype(jnp.int32), axis=1)
    return (flat * cap + ranks).reshape(top, rows)


def send_places(experts, cap, swap):
    p = jnp.arange(experts * 24, dtype=jnp.int32)
    e, piece, r = p // 24, p % 24 // 8, p % 8
    rank = jnp.where(piece < 2, r, 8 + r % 4)
    half = jnp.where(piece < 2, piece, r // 4)
    if swap:
        half = jnp.where(e % 2 == 1, 1 - half, half)
    return e * cap + rank, half


RIGHT = [(i, (i + 1) % 4) for i in range(4)]
LEFT = [(i, (i - 1) % 4) for i in range(4)]


def first_hop(shard):
    return lax.ppermute(shard, "x", RIGHT), lax.ppermute(shard, "x", LEFT)


def second_hop(before, after):
    half = before.shape[0] // 2
    return lax.ppermute(before[:half], "x", RIGHT), lax.ppermute(after[half:], "x", LEFT)


def weight_products(where_ref, x_ref, pieces):
    x, zl = where_ref[0], where_ref[1]
    width = x_ref.shape[1] // 8
    total = None
    for n, piece in enumerate(pieces):
        line = zl if n < 4 else 1 - zl
        at = pl.multiple_of((line * 4 + (x + (0, 3, 1, 2)[n % 4]) % 4) * width, width)
        product = dot(x_ref[:, pl.ds(at, width)], piece[...])
        total = product if total is None else total + product
    return total


def half_kernel(where_ref, x_ref, first_ref, *refs):
    frozen_ref, low_ref = refs[8:]
    frozen_ref[...] = weight_products(where_ref, x_ref, refs[:8])
    low_ref[...] = dot(x_ref[...], first_ref[...], ((1,), (1,)))


def final_kernel(where_ref, xa_ref, xb_ref, g0_ref, g1_ref, frozen_ref, lowa_ref, first_ref, second_ref, *refs):
    out_ref, frozen_acc, slope_acc, sums = refs[8:]
    step = pl.program_id(0)
    low = (lowa_ref[...] + dot(xb_ref[...], first_ref[...], ((1,), (1,)))).astype(jnp.bfloat16)
    frozen_acc[...] = frozen_ref[...] + weight_products(where_ref, xb_ref, refs[:8])
    half = g0_ref.shape[1]
    for h, g_ref in enumerate((g0_ref, g1_ref)):
        cols = slice(h * half, (h + 1) * half)
        preact = frozen_acc[:, cols] + ADAPTER_SCALE * dot(low, second_ref[:, cols])
        slope = g_ref[...].astype(jnp.float32) * silu_slope(preact)
        slope_acc[:, cols] = slope.astype(jnp.bfloat16)
    back = dot(slope_acc[...], second_ref[...], ((1,), (1,))).astype(jnp.bfloat16)

    @pl.when(step == 0)
    def _():
        sums[...] = jnp.zeros_like(sums)

    width = xa_ref.shape[1] // 8
    for h, x_ref in enumerate((xa_ref, xb_ref)):
        part = dot(back, x_ref[...], ((0,), (0,)))
        for n in range(8):
            at = (2 * n + h) * width
            sums[:, at : at + width] += part[:, n * width : (n + 1) * width]
    sums[:, 16 * width :] += dot(low, slope_acc[...], ((0,), (0,)))

    @pl.when(step == pl.num_programs(0) - 1)
    def _():
        chunk = out_ref.shape[2]
        for n in range(4):
            out_ref[n] = ADAPTER_SCALE * sums[:, n * chunk : (n + 1) * chunk]


ROW_BLOCK = 256


def row_spec(array):
    return pl.BlockSpec((ROW_BLOCK, array.shape[1]), lambda i, w: (i, 0))


def whole_spec(array):
    return pl.BlockSpec(array.shape, lambda i, w: (0, 0))


def piece_specs(pieces, h):
    specs = []
    for piece in pieces:
        at = h if piece.shape[0] == 512 else 0
        specs.append(pl.BlockSpec((256, piece.shape[1]), lambda i, w, at=at: (at, 0)))
    return specs


def half_products(where, x, first, pieces, h):
    rows, hidden, rank = x.shape[0], pieces[0].shape[1], first.shape[0]
    return pl.pallas_call(
        half_kernel,
        grid_spec=pltpu.PrefetchScalarGridSpec(
            num_scalar_prefetch=1,
            grid=(rows // ROW_BLOCK,),
            in_specs=[row_spec(x), whole_spec(first)] + piece_specs(pieces, h),
            out_specs=[
                pl.BlockSpec((ROW_BLOCK, hidden), lambda i, w: (i, 0)),
                pl.BlockSpec((ROW_BLOCK, rank), lambda i, w: (i, 0)),
            ],
        ),
        out_shape=[
            jax.ShapeDtypeStruct((rows, hidden), jnp.float32),
            jax.ShapeDtypeStruct((rows, rank), jnp.float32),
        ],
        name="half_products",
    )(where, x, first, *pieces)


def gradients(where, xa, xb, g0, g1, frozen, low, first, second, pieces, h):
    rows, hidden, rank = xa.shape[0], pieces[0].shape[1], first.shape[0]
    total = 2 * xa.shape[1] + hidden
    by_row = [row_spec(v) for v in (xa, xb, g0, g1, frozen, low)]
    return pl.pallas_call(
        final_kernel,
        grid_spec=pltpu.PrefetchScalarGridSpec(
            num_scalar_prefetch=1,
            grid=(rows // ROW_BLOCK,),
            in_specs=by_row + [whole_spec(first), whole_spec(second)] + piece_specs(pieces, h),
            out_specs=pl.BlockSpec((4, rank, total // 4), lambda i, w: (0, 0, 0)),
            scratch_shapes=[
                pltpu.VMEM((ROW_BLOCK, hidden), jnp.float32),
                pltpu.VMEM((ROW_BLOCK, hidden), jnp.bfloat16),
                pltpu.VMEM((rank, total), jnp.float32),
            ],
        ),
        out_shape=jax.ShapeDtypeStruct((4, rank, total // 4), jnp.float32),
        name="gradients",
    )(where, xa, xb, g0, g1, frozen, low, first, second, *pieces)


def split_kernel(tokens_ref, *out_refs):
    for h, out_ref in enumerate(out_refs):
        for n in range(out_ref.shape[1] // 256):
            at = (2 * n + h) * 256
            out_ref[:, n * 256 : (n + 1) * 256] = tokens_ref[:, at : at + 256]


def split_columns(tokens):
    shape = jax.ShapeDtypeStruct((tokens.shape[0], tokens.shape[1] // 2), tokens.dtype)
    return pl.pallas_call(split_kernel, out_shape=[shape, shape], name="split_columns")(tokens)


def local(tokens, route, gate_output_gradient, frozen_gate_weight, adapter_first, adapter_second):
    tok_rows, width = tokens.shape
    hidden = gate_output_gradient.shape[2]
    experts = 64
    cap = 12
    depth = 8
    zh, zl, x = lax.axis_index("zh"), lax.axis_index("zl"), lax.axis_index("x")
    half_width = width // 2

    lines = [
        lax.all_gather(part, ("zh", "zl"), axis=0, tiled=True) for part in split_columns(tokens)
    ]

    target = slot_targets(route, cap)
    line_target = jnp.broadcast_to(target[None], (depth, 2, tok_rows))
    line_target = lax.all_to_all(line_target, ("zh", "zl"), split_axis=0, concat_axis=0, tiled=True)

    mine = lax.dynamic_index_in_dim(frozen_gate_weight, zl, 0, keepdims=False)
    other = lax.dynamic_index_in_dim(frozen_gate_weight, 1 - zl, 0, keepdims=False)
    near = first_hop(mine)
    other, line_target = lax.optimization_barrier((other, line_target))
    got = lax.ppermute(other, "zl", [(0, 1), (1, 0)])

    place, half = send_places(experts, cap, False)
    match = place[:, None] == target.reshape(1, 2 * tok_rows)
    pick_g = jnp.concatenate([match & (half == 0)[:, None], match & (half == 1)[:, None]], axis=1)
    half_hidden = hidden // 2
    parts = [
        gate_output_gradient[:, k, h * half_hidden : (h + 1) * half_hidden]
        for h in range(2)
        for k in range(2)
    ]
    send_g = dot(pick_g.astype(jnp.bfloat16), jnp.concatenate(parts, axis=0)).astype(jnp.bfloat16)
    send_g = send_g.reshape(experts, 24, half_hidden)
    send_g, line_target = lax.optimization_barrier((send_g, line_target))
    recv_g = lax.all_to_all(send_g, PLANE, split_axis=0, concat_axis=0, tiled=True)

    line_target = line_target.transpose(1, 0, 2).reshape(2, depth * tok_rows)
    row = jnp.arange(depth * depth * cap, dtype=jnp.int32)
    served = (zh * depth + row // (depth * cap)) * 2 + zl
    key = (served * cap + row % cap)[:, None]
    col = jnp.arange(depth * tok_rows, dtype=jnp.int32)
    same_block = (row // cap % depth)[:, None] == (col // tok_rows)[None, :]
    pick = same_block & ((line_target[0][None] == key) | (line_target[1][None] == key))
    pick = pick.astype(jnp.bfloat16)

    def packed(line):
        return dot(pick, line).astype(jnp.bfloat16).reshape(depth, depth * cap, half_width)

    def spread(rows):
        rows = lax.all_to_all(rows, ("y", "c"), split_axis=0, concat_axis=0, tiled=True)
        return rows.reshape(depth * depth * cap, half_width)

    near_opposite = second_hop(*near)
    line0, near_opposite = lax.optimization_barrier((lines[0], near_opposite))
    send_0, recv_g, got = lax.optimization_barrier((packed(line0), recv_g, got))
    far = first_hop(got)
    xa = spread(send_0)
    line1, far = lax.optimization_barrier((lines[1], far))
    far_opposite = second_hop(*far)
    xb = spread(packed(line1))

    recv_g = recv_g.reshape(experts * 24, half_hidden)
    block, rank = row // cap, row % cap
    source = block // 2 % 4 * 16 + block // 8 * 2 + block % 2
    q = jnp.arange(experts * 24, dtype=jnp.int32)

    def gather_half(h):
        at = source * 24 + jnp.where(rank < 8, 8 * h + rank, 16 + 4 * h + rank - 8)
        return dot((at[:, None] == q[None, :]).astype(jnp.bfloat16), recv_g).astype(jnp.bfloat16)

    first = lax.dynamic_index_in_dim(adapter_first, zl, 0, keepdims=False)
    second = lax.dynamic_index_in_dim(adapter_second, zl, 0, keepdims=False)
    first = first.T
    first_a, first_b = (
        jnp.concatenate([first[:, at : at + 256] for at in range(256 * h, width, 512)], axis=1)
        for h in range(2)
    )
    where = jnp.stack([x, zl]).astype(jnp.int32)
    pieces = [
        [mine, *near, near_opposite[h], got, *far, far_opposite[h]]
        for h in range(2)
    ]
    frozen, low = half_products(where, xa, first_a, pieces[0], 0)
    parts = gradients(
        where, xa, xb, gather_half(0), gather_half(1), frozen, low, first_b, second, pieces[1], 1
    )

    rank, chunk = parts.shape[1:]
    parts = lax.all_to_all(parts, "x", split_axis=0, concat_axis=0, tiled=True)
    total = jnp.sum(parts, axis=0).astype(jnp.bfloat16)
    total = jnp.broadcast_to(total[None], (8, rank, chunk))
    total = lax.all_to_all(total, DP_AXES, split_axis=0, concat_axis=0, tiled=True)
    total = total.reshape(2, 4, rank, chunk).transpose(0, 2, 1, 3).reshape(2, rank, 4 * chunk)
    grad_a = total[:, :, :width].transpose(0, 2, 1).astype(jnp.float32)
    return grad_a, total[:, :, width:].astype(jnp.float32)


def solution(mesh):
    fine = Mesh(mesh.devices.reshape(4, 4, 2, 2, 4), EXPERT_AXES + DP_AXES)
    everyone = EXPERT_AXES + DP_AXES

    def step(*args):
        return local(*args)

    step = jax.shard_map(
        step,
        mesh=fine,
        in_specs=(
            P(everyone, None),
            P(everyone, None),
            P(everyone, None, None),
            P(EXPERT_AXES, DP_AXES, None),
            P(EXPERT_AXES, None, None),
            P(EXPERT_AXES, None, None),
        ),
        out_specs=(P(EXPERT_AXES, None, None), P(EXPERT_AXES, None, None)),
        check_vma=False,
    )
    return step
```

```python
import jax
import jax.numpy as jnp
from jax import lax
from jax.experimental import pallas as pl
from jax.experimental.pallas import tpu as pltpu
from jax.sharding import Mesh, PartitionSpec as P


ADAPTER_SCALE = 2.0
EXPERT_AXES = ("zh", "y", "c")
DP_AXES = ("zl", "x")


def dot(a, b, dims=((1,), (0,))):
    return lax.dot_general(a, b, (dims, ((), ())), preferred_element_type=jnp.float32)


def silu_slope(gate_preactivation):
    squash = jax.nn.sigmoid(gate_preactivation)
    return squash * (1.0 + gate_preactivation * (1.0 - squash))


def slot_targets(route, cap):
    rows, top = route.shape
    flat = route.T.reshape(rows * top)
    before = jnp.arange(rows * top)[:, None] > jnp.arange(rows * top)[None, :]
    same = flat[:, None] == flat[None, :]
    ranks = jnp.sum((same & before).astype(jnp.int32), axis=1)
    return (flat * cap + ranks).reshape(top, rows)


RIGHT = [(i, (i + 1) % 4) for i in range(4)]
LEFT = [(i, (i - 1) % 4) for i in range(4)]


def first_hop(shard):
    return lax.ppermute(shard, "x", RIGHT), lax.ppermute(shard, "x", LEFT)


def second_hop(before, after):
    half = before.shape[0] // 2
    return lax.ppermute(before[:half], "x", RIGHT), lax.ppermute(after[half:], "x", LEFT)


def weight_products(where_ref, x_ref, pieces):
    x, zl = where_ref[0], where_ref[1]
    width = x_ref.shape[1] // 8
    total = None
    for n, piece in enumerate(pieces):
        line = zl if n < 4 else 1 - zl
        at = pl.multiple_of((line * 4 + (x + (0, 3, 1, 2)[n % 4]) % 4) * width, width)
        product = dot(x_ref[:, pl.ds(at, width)], piece[...])
        total = product if total is None else total + product
    return total


def half_kernel(where_ref, x_ref, first_ref, *refs):
    frozen_ref, low_ref = refs[8:]
    frozen_ref[...] = weight_products(where_ref, x_ref, refs[:8])
    low_ref[...] = dot(x_ref[...], first_ref[...], ((1,), (1,)))


def final_kernel(where_ref, xa_ref, xb_ref, g_ref, frozen_ref, lowa_ref, first_ref, second_ref, *refs):
    out_ref, frozen_acc, slope_acc, sums = refs[8:]
    step = pl.program_id(0)
    low = (lowa_ref[...] + dot(xb_ref[...], first_ref[...], ((1,), (1,)))).astype(jnp.bfloat16)
    frozen_acc[...] = frozen_ref[...] + weight_products(where_ref, xb_ref, refs[:8])
    half = g_ref.shape[1] // 2
    for h in range(2):
        cols = slice(h * half, (h + 1) * half)
        preact = frozen_acc[:, cols] + ADAPTER_SCALE * dot(low, second_ref[:, cols])
        slope = g_ref[:, cols].astype(jnp.float32) * silu_slope(preact)
        slope_acc[:, cols] = slope.astype(jnp.bfloat16)
    back = dot(slope_acc[...], second_ref[...], ((1,), (1,))).astype(jnp.bfloat16)

    @pl.when(step == 0)
    def _():
        sums[...] = jnp.zeros_like(sums)

    width = xa_ref.shape[1] // 8
    for h, x_ref in enumerate((xa_ref, xb_ref)):
        part = dot(back, x_ref[...], ((0,), (0,)))
        for n in range(8):
            at = (2 * n + h) * width
            sums[:, at : at + width] += part[:, n * width : (n + 1) * width]
    sums[:, 16 * width :] += dot(low, slope_acc[...], ((0,), (0,)))

    @pl.when(step == pl.num_programs(0) - 1)
    def _():
        chunk = out_ref.shape[2]
        for n in range(4):
            out_ref[n] = ADAPTER_SCALE * sums[:, n * chunk : (n + 1) * chunk]


ROW_BLOCK = 256


def row_spec(array):
    return pl.BlockSpec((ROW_BLOCK, array.shape[1]), lambda i, w: (i, 0))


def whole_spec(array):
    return pl.BlockSpec(array.shape, lambda i, w: (0, 0))


def piece_specs(pieces, h):
    specs = []
    for piece in pieces:
        at = h if piece.shape[0] == 512 else 0
        specs.append(pl.BlockSpec((256, piece.shape[1]), lambda i, w, at=at: (at, 0)))
    return specs


def half_products(where, x, first, pieces, h):
    rows, hidden, rank = x.shape[0], pieces[0].shape[1], first.shape[0]
    return pl.pallas_call(
        half_kernel,
        grid_spec=pltpu.PrefetchScalarGridSpec(
            num_scalar_prefetch=1,
            grid=(rows // ROW_BLOCK,),
            in_specs=[row_spec(x), whole_spec(first)] + piece_specs(pieces, h),
            out_specs=[
                pl.BlockSpec((ROW_BLOCK, hidden), lambda i, w: (i, 0)),
                pl.BlockSpec((ROW_BLOCK, rank), lambda i, w: (i, 0)),
            ],
        ),
        out_shape=[
            jax.ShapeDtypeStruct((rows, hidden), jnp.float32),
            jax.ShapeDtypeStruct((rows, rank), jnp.float32),
        ],
        name="half_products",
    )(where, x, first, *pieces)


def gradients(where, xa, xb, g, frozen, low, first, second, pieces, h):
    rows, hidden, rank = xa.shape[0], pieces[0].shape[1], first.shape[0]
    total = 2 * xa.shape[1] + hidden
    by_row = [row_spec(v) for v in (xa, xb, g, frozen, low)]
    return pl.pallas_call(
        final_kernel,
        grid_spec=pltpu.PrefetchScalarGridSpec(
            num_scalar_prefetch=1,
            grid=(rows // ROW_BLOCK,),
            in_specs=by_row + [whole_spec(first), whole_spec(second)] + piece_specs(pieces, h),
            out_specs=pl.BlockSpec((4, rank, total // 4), lambda i, w: (0, 0, 0)),
            scratch_shapes=[
                pltpu.VMEM((ROW_BLOCK, hidden), jnp.float32),
                pltpu.VMEM((ROW_BLOCK, hidden), jnp.bfloat16),
                pltpu.VMEM((rank, total), jnp.float32),
            ],
        ),
        out_shape=jax.ShapeDtypeStruct((4, rank, total // 4), jnp.float32),
        name="gradients",
    )(where, xa, xb, g, frozen, low, first, second, *pieces)


def split_kernel(tokens_ref, *out_refs):
    for h, out_ref in enumerate(out_refs):
        for n in range(out_ref.shape[1] // 256):
            at = (2 * n + h) * 256
            out_ref[:, n * 256 : (n + 1) * 256] = tokens_ref[:, at : at + 256]


def split_columns(tokens):
    shape = jax.ShapeDtypeStruct((tokens.shape[0], tokens.shape[1] // 2), tokens.dtype)
    return pl.pallas_call(split_kernel, out_shape=[shape, shape], name="split_columns")(tokens)


def local(tokens, route, gate_output_gradient, frozen_gate_weight, adapter_first, adapter_second):
    tok_rows, width = tokens.shape
    hidden = gate_output_gradient.shape[2]
    cap = 12
    depth = 8
    zh, zl, x = lax.axis_index("zh"), lax.axis_index("zl"), lax.axis_index("x")
    half_width = width // 2

    lines = [
        lax.all_gather(part, ("zh", "zl"), axis=0, tiled=True) for part in split_columns(tokens)
    ]

    target = slot_targets(route, cap)
    line_target = jnp.broadcast_to(target[None], (depth, 2, tok_rows))
    line_target = lax.all_to_all(line_target, ("zh", "zl"), split_axis=0, concat_axis=0, tiled=True)

    mine = lax.dynamic_index_in_dim(frozen_gate_weight, zl, 0, keepdims=False)
    other = lax.dynamic_index_in_dim(frozen_gate_weight, 1 - zl, 0, keepdims=False)
    near = first_hop(mine)
    other, line_target = lax.optimization_barrier((other, line_target))
    got = lax.ppermute(other, "zl", [(0, 1), (1, 0)])

    row = jnp.arange(depth * depth * cap, dtype=jnp.int32)
    outer, inner, rank = row // (depth * cap), row // cap % depth, row % cap
    zi = zh * 2 + zl
    ahead = (zi + inner) % depth
    key = ((ahead // 2 * depth + outer) * 2 + ahead % 2) * cap + rank
    pick_g = key[:, None] == target.reshape(1, 2 * tok_rows)
    slots = jnp.concatenate([gate_output_gradient[:, k] for k in range(2)], axis=0)
    send_g = dot(pick_g.astype(jnp.bfloat16), slots).astype(jnp.bfloat16)
    send_g = send_g.reshape(depth, depth * cap, hidden)
    send_g, line_target = lax.optimization_barrier((send_g, line_target))
    column_g = lax.all_to_all(send_g, ("y", "c"), split_axis=0, concat_axis=0, tiled=True)
    swapped = (inner * depth + outer) * cap + rank
    swap = (swapped[:, None] == row[None, :]).astype(jnp.bfloat16)
    column_g = dot(swap, column_g.reshape(-1, hidden)).astype(jnp.bfloat16)
    blocks_g = [column_g[n * depth * cap : (n + 1) * depth * cap] for n in range(depth)]
    for n in (4, 3, 5, 2, 6, 1, 7):
        moves = [(i, (i + n) % depth) for i in range(depth)]
        blocks_g[n] = lax.ppermute(blocks_g[n], ("zh", "zl"), moves)

    line_target = line_target.transpose(1, 0, 2).reshape(2, depth * tok_rows)
    served = (zh * depth + outer) * 2 + zl
    key = (served * cap + row % cap)[:, None]
    col = jnp.arange(depth * tok_rows, dtype=jnp.int32)
    same_block = (row // cap % depth)[:, None] == (col // tok_rows)[None, :]
    pick = same_block & ((line_target[0][None] == key) | (line_target[1][None] == key))
    pick = pick.astype(jnp.bfloat16)

    def packed(line):
        return dot(pick, line).astype(jnp.bfloat16).reshape(depth, depth * cap, half_width)

    def spread(rows):
        rows = lax.all_to_all(rows, ("y", "c"), split_axis=0, concat_axis=0, tiled=True)
        return rows.reshape(depth * depth * cap, half_width)

    near_opposite = second_hop(*near)
    line0, near_opposite, column_g = lax.optimization_barrier((lines[0], near_opposite, column_g))
    far = first_hop(got)
    send_0, far = lax.optimization_barrier((packed(line0), far))
    far_opposite = second_hop(*far)
    xa = spread(send_0)
    line1, far_opposite = lax.optimization_barrier((lines[1], far_opposite))
    xb = spread(packed(line1))

    behind = (zi - inner) % depth
    order = (behind * depth + outer) * cap + rank
    order = (order[:, None] == row[None, :]).astype(jnp.bfloat16)
    rows_g = dot(order, jnp.concatenate(blocks_g, axis=0)).astype(jnp.bfloat16)

    first = lax.dynamic_index_in_dim(adapter_first, zl, 0, keepdims=False)
    second = lax.dynamic_index_in_dim(adapter_second, zl, 0, keepdims=False)
    first = first.T
    first_a, first_b = (
        jnp.concatenate([first[:, at : at + 256] for at in range(256 * h, width, 512)], axis=1)
        for h in range(2)
    )
    where = jnp.stack([x, zl]).astype(jnp.int32)
    pieces = [
        [mine, *near, near_opposite[h], got, *far, far_opposite[h]]
        for h in range(2)
    ]
    frozen, low = half_products(where, xa, first_a, pieces[0], 0)
    parts = gradients(where, xa, xb, rows_g, frozen, low, first_b, second, pieces[1], 1)

    rank, chunk = parts.shape[1:]
    parts = lax.all_to_all(parts, "x", split_axis=0, concat_axis=0, tiled=True)
    total = jnp.sum(parts, axis=0).astype(jnp.bfloat16)
    total = jnp.broadcast_to(total[None], (8, rank, chunk))
    total = lax.all_to_all(total, DP_AXES, split_axis=0, concat_axis=0, tiled=True)
    total = total.reshape(2, 4, rank, chunk).transpose(0, 2, 1, 3).reshape(2, rank, 4 * chunk)
    grad_a = total[:, :, :width].transpose(0, 2, 1).astype(jnp.float32)
    return grad_a, total[:, :, width:].astype(jnp.float32)


def solution(mesh):
    fine = Mesh(mesh.devices.reshape(4, 4, 2, 2, 4), EXPERT_AXES + DP_AXES)
    everyone = EXPERT_AXES + DP_AXES

    def step(*args):
        return local(*args)

    step = jax.shard_map(
        step,
        mesh=fine,
        in_specs=(
            P(everyone, None),
            P(everyone, None),
            P(everyone, None, None),
            P(EXPERT_AXES, DP_AXES, None),
            P(EXPERT_AXES, None, None),
            P(EXPERT_AXES, None, None),
        ),
        out_specs=(P(EXPERT_AXES, None, None), P(EXPERT_AXES, None, None)),
        check_vma=False,
    )
    return step
```

```python
import jax
import jax.numpy as jnp
from jax import lax
from jax.experimental import pallas as pl
from jax.experimental.pallas import tpu as pltpu
from jax.sharding import Mesh, PartitionSpec as P


ADAPTER_SCALE = 2.0
EXPERT_AXES = ("zh", "y", "c")
DP_AXES = ("zl", "x")


def dot(a, b, dims=((1,), (0,))):
    return lax.dot_general(a, b, (dims, ((), ())), preferred_element_type=jnp.float32)


def silu_slope(gate_preactivation):
    squash = jax.nn.sigmoid(gate_preactivation)
    return squash * (1.0 + gate_preactivation * (1.0 - squash))


def slot_targets(route, cap):
    rows, top = route.shape
    flat = route.T.reshape(rows * top)
    before = jnp.arange(rows * top)[:, None] > jnp.arange(rows * top)[None, :]
    same = flat[:, None] == flat[None, :]
    ranks = jnp.sum((same & before).astype(jnp.int32), axis=1)
    return (flat * cap + ranks).reshape(top, rows)


RIGHT = [(i, (i + 1) % 4) for i in range(4)]
LEFT = [(i, (i - 1) % 4) for i in range(4)]


def first_hop(shard):
    return lax.ppermute(shard, "x", RIGHT), lax.ppermute(shard, "x", LEFT)


def second_hop(before, after):
    half = before.shape[0] // 2
    return lax.ppermute(before[:half], "x", RIGHT), lax.ppermute(after[half:], "x", LEFT)


def join_weights(where_ref, pieces, weight):
    x, zl = where_ref[0], where_ref[1]
    rows = weight.shape[0] // 8

    @pl.when(pl.program_id(0) == 0)
    def _():
        for n, piece in enumerate(pieces):
            line = zl if n < 4 else 1 - zl
            at = pl.multiple_of((line * 4 + (x + (0, 3, 1, 2)[n % 4]) % 4) * rows, rows)
            weight[pl.ds(at, rows), :] = piece[...]


def half_kernel(where_ref, x_ref, first_ref, *refs):
    frozen_ref, low_ref, weight = refs[8:]
    join_weights(where_ref, refs[:8], weight)
    frozen_ref[...] = dot(x_ref[...], weight[...])
    low_ref[...] = dot(x_ref[...], first_ref[...], ((1,), (1,)))


def final_kernel(where_ref, xa_ref, xb_ref, g_ref, frozen_ref, lowa_ref, first_ref, second_ref, *refs):
    out_ref, frozen_acc, slope_acc, sums, weight = refs[8:]
    join_weights(where_ref, refs[:8], weight)
    step = pl.program_id(0)
    low = (lowa_ref[...] + dot(xb_ref[...], first_ref[...], ((1,), (1,)))).astype(jnp.bfloat16)
    frozen_acc[...] = frozen_ref[...] + dot(xb_ref[...], weight[...])
    half = g_ref.shape[1] // 2
    for h in range(2):
        cols = slice(h * half, (h + 1) * half)
        preact = frozen_acc[:, cols] + ADAPTER_SCALE * dot(low, second_ref[:, cols])
        slope = g_ref[:, cols].astype(jnp.float32) * silu_slope(preact)
        slope_acc[:, cols] = slope.astype(jnp.bfloat16)
    back = dot(slope_acc[...], second_ref[...], ((1,), (1,))).astype(jnp.bfloat16)

    @pl.when(step == 0)
    def _():
        sums[...] = jnp.zeros_like(sums)

    width = xa_ref.shape[1] // 8
    for h, x_ref in enumerate((xa_ref, xb_ref)):
        part = dot(back, x_ref[...], ((0,), (0,)))
        for n in range(8):
            at = (2 * n + h) * width
            sums[:, at : at + width] += part[:, n * width : (n + 1) * width]
    sums[:, 16 * width :] += dot(low, slope_acc[...], ((0,), (0,)))

    @pl.when(step == pl.num_programs(0) - 1)
    def _():
        chunk = out_ref.shape[2]
        for n in range(4):
            out_ref[n] = ADAPTER_SCALE * sums[:, n * chunk : (n + 1) * chunk]


ROW_BLOCK = 256


def row_spec(array):
    return pl.BlockSpec((ROW_BLOCK, array.shape[1]), lambda i, w: (i, 0))


def whole_spec(array):
    return pl.BlockSpec(array.shape, lambda i, w: (0, 0))


def piece_specs(pieces, h):
    specs = []
    for piece in pieces:
        at = h if piece.shape[0] == 512 else 0
        specs.append(pl.BlockSpec((256, piece.shape[1]), lambda i, w, at=at: (at, 0)))
    return specs


def half_products(where, x, first, pieces, h):
    rows, hidden, rank = x.shape[0], pieces[0].shape[1], first.shape[0]
    return pl.pallas_call(
        half_kernel,
        grid_spec=pltpu.PrefetchScalarGridSpec(
            num_scalar_prefetch=1,
            grid=(rows // ROW_BLOCK,),
            in_specs=[row_spec(x), whole_spec(first)] + piece_specs(pieces, h),
            out_specs=[
                pl.BlockSpec((ROW_BLOCK, hidden), lambda i, w: (i, 0)),
                pl.BlockSpec((ROW_BLOCK, rank), lambda i, w: (i, 0)),
            ],
            scratch_shapes=[pltpu.VMEM((x.shape[1], hidden), jnp.bfloat16)],
        ),
        cost_estimate=pl.CostEstimate(
            flops=2 * rows * x.shape[1] * hidden, bytes_accessed=14 * 2**20, transcendentals=0
        ),
        out_shape=[
            jax.ShapeDtypeStruct((rows, hidden), jnp.float32),
            jax.ShapeDtypeStruct((rows, rank), jnp.float32),
        ],
        name="half_products",
    )(where, x, first, *pieces)


def gradients(where, xa, xb, g, frozen, low, first, second, pieces, h):
    rows, hidden, rank = xa.shape[0], pieces[0].shape[1], first.shape[0]
    total = 2 * xa.shape[1] + hidden
    by_row = [row_spec(v) for v in (xa, xb, g, frozen, low)]
    return pl.pallas_call(
        final_kernel,
        grid_spec=pltpu.PrefetchScalarGridSpec(
            num_scalar_prefetch=1,
            grid=(rows // ROW_BLOCK,),
            in_specs=by_row + [whole_spec(first), whole_spec(second)] + piece_specs(pieces, h),
            out_specs=pl.BlockSpec((4, rank, total // 4), lambda i, w: (0, 0, 0)),
            scratch_shapes=[
                pltpu.VMEM((ROW_BLOCK, hidden), jnp.float32),
                pltpu.VMEM((ROW_BLOCK, hidden), jnp.bfloat16),
                pltpu.VMEM((rank, total), jnp.float32),
                pltpu.VMEM((xa.shape[1], hidden), jnp.bfloat16),
            ],
        ),
        out_shape=jax.ShapeDtypeStruct((4, rank, total // 4), jnp.float32),
        name="gradients",
    )(where, xa, xb, g, frozen, low, first, second, *pieces)


def split_kernel(tokens_ref, *out_refs):
    for h, out_ref in enumerate(out_refs):
        for n in range(out_ref.shape[1] // 256):
            at = (2 * n + h) * 256
            out_ref[:, n * 256 : (n + 1) * 256] = tokens_ref[:, at : at + 256]


def split_columns(tokens):
    shape = jax.ShapeDtypeStruct((tokens.shape[0], tokens.shape[1] // 2), tokens.dtype)
    return pl.pallas_call(split_kernel, out_shape=[shape, shape], name="split_columns")(tokens)


def local(tokens, route, gate_output_gradient, frozen_gate_weight, adapter_first, adapter_second):
    tok_rows, width = tokens.shape
    hidden = gate_output_gradient.shape[2]
    cap = 12
    depth = 8
    zh, zl, x = lax.axis_index("zh"), lax.axis_index("zl"), lax.axis_index("x")
    half_width = width // 2

    lines = [
        lax.all_gather(part, ("zh", "zl"), axis=0, tiled=True) for part in split_columns(tokens)
    ]

    target = slot_targets(route, cap)
    line_target = jnp.broadcast_to(target[None], (depth, 2, tok_rows))
    line_target = lax.all_to_all(line_target, ("zh", "zl"), split_axis=0, concat_axis=0, tiled=True)

    mine = lax.dynamic_index_in_dim(frozen_gate_weight, zl, 0, keepdims=False)
    other = lax.dynamic_index_in_dim(frozen_gate_weight, 1 - zl, 0, keepdims=False)
    near = first_hop(mine)
    other, line_target = lax.optimization_barrier((other, line_target))
    got = lax.ppermute(other, "zl", [(0, 1), (1, 0)])

    row = jnp.arange(depth * depth * cap, dtype=jnp.int32)
    outer, inner, rank = row // (depth * cap), row // cap % depth, row % cap
    zi = zh * 2 + zl
    ahead = (zi + inner) % depth
    key = ((ahead // 2 * depth + outer) * 2 + ahead % 2) * cap + rank
    pick_g = key[:, None] == target.reshape(1, 2 * tok_rows)
    slots = jnp.concatenate([gate_output_gradient[:, k] for k in range(2)], axis=0)
    send_g = dot(pick_g.astype(jnp.bfloat16), slots).astype(jnp.bfloat16)
    send_g = send_g.reshape(depth, depth * cap, hidden)
    send_g, line_target = lax.optimization_barrier((send_g, line_target))
    column_g = lax.all_to_all(send_g, ("y", "c"), split_axis=0, concat_axis=0, tiled=True)
    swapped = (inner * depth + outer) * cap + rank
    swap = (swapped[:, None] == row[None, :]).astype(jnp.bfloat16)
    column_g = dot(swap, column_g.reshape(-1, hidden)).astype(jnp.bfloat16)

    line_target = line_target.transpose(1, 0, 2).reshape(2, depth * tok_rows)
    served = (zh * depth + outer) * 2 + zl
    key = (served * cap + row % cap)[:, None]
    col = jnp.arange(depth * tok_rows, dtype=jnp.int32)
    same_block = (row // cap % depth)[:, None] == (col // tok_rows)[None, :]
    pick = same_block & ((line_target[0][None] == key) | (line_target[1][None] == key))
    pick = pick.astype(jnp.bfloat16)

    def packed(line):
        return dot(pick, line).astype(jnp.bfloat16).reshape(depth, depth * cap, half_width)

    def spread(rows):
        rows = lax.all_to_all(rows, ("y", "c"), split_axis=0, concat_axis=0, tiled=True)
        return rows.reshape(depth * depth * cap, half_width)

    near_opposite = second_hop(*near)
    got, near_opposite, column_g = lax.optimization_barrier((got, near_opposite, column_g))
    far = first_hop(got)
    line0, near_opposite = lax.optimization_barrier((lines[0], near_opposite))
    xa = spread(packed(line0))
    far_opposite = second_hop(*far)
    blocks_g = [column_g[n * depth * cap : (n + 1) * depth * cap] for n in range(depth)]
    line1, far_opposite, blocks_g = lax.optimization_barrier((lines[1], far_opposite, blocks_g))
    for n in (4, 5, 3, 6, 2, 7, 1):
        moves = [(i, (i + n) % depth) for i in range(depth)]
        blocks_g[n] = lax.ppermute(blocks_g[n], ("zh", "zl"), moves)
    xb = spread(packed(line1))

    behind = (zi - inner) % depth
    order = (behind * depth + outer) * cap + rank
    order = (order[:, None] == row[None, :]).astype(jnp.bfloat16)
    rows_g = dot(order, jnp.concatenate(blocks_g, axis=0)).astype(jnp.bfloat16)

    first = lax.dynamic_index_in_dim(adapter_first, zl, 0, keepdims=False)
    second = lax.dynamic_index_in_dim(adapter_second, zl, 0, keepdims=False)
    first = first.T
    first_a, first_b = (
        jnp.concatenate([first[:, at : at + 256] for at in range(256 * h, width, 512)], axis=1)
        for h in range(2)
    )
    where = jnp.stack([x, zl]).astype(jnp.int32)
    pieces = [
        [mine, *near, near_opposite[h], got, *far, far_opposite[h]]
        for h in range(2)
    ]
    frozen, low = half_products(where, xa, first_a, pieces[0], 0)
    parts = gradients(where, xa, xb, rows_g, frozen, low, first_b, second, pieces[1], 1)

    rank, chunk = parts.shape[1:]
    parts = lax.all_to_all(parts, "x", split_axis=0, concat_axis=0, tiled=True)
    total = jnp.sum(parts, axis=0).astype(jnp.bfloat16)
    total = jnp.broadcast_to(total[None], (8, rank, chunk))
    total = lax.all_to_all(total, DP_AXES, split_axis=0, concat_axis=0, tiled=True)
    total = total.reshape(2, 4, rank, chunk).transpose(0, 2, 1, 3).reshape(2, rank, 4 * chunk)
    grad_a = total[:, :, :width].transpose(0, 2, 1).astype(jnp.float32)
    return grad_a, total[:, :, width:].astype(jnp.float32)


def solution(mesh):
    fine = Mesh(mesh.devices.reshape(4, 4, 2, 2, 4), EXPERT_AXES + DP_AXES)
    everyone = EXPERT_AXES + DP_AXES

    def step(*args):
        return local(*args)

    step = jax.shard_map(
        step,
        mesh=fine,
        in_specs=(
            P(everyone, None),
            P(everyone, None),
            P(everyone, None, None),
            P(EXPERT_AXES, DP_AXES, None),
            P(EXPERT_AXES, None, None),
            P(EXPERT_AXES, None, None),
        ),
        out_specs=(P(EXPERT_AXES, None, None), P(EXPERT_AXES, None, None)),
        check_vma=False,
    )
    return step
```

```python
import jax
import jax.numpy as jnp
from jax import lax
from jax.experimental import pallas as pl
from jax.experimental.pallas import tpu as pltpu
from jax.sharding import Mesh, PartitionSpec as P


ADAPTER_SCALE = 2.0
EXPERT_AXES = ("zh", "y", "c")
DP_AXES = ("zl", "x")


def dot(a, b, dims=((1,), (0,))):
    return lax.dot_general(a, b, (dims, ((), ())), preferred_element_type=jnp.float32)


def silu_slope(gate_preactivation):
    squash = jax.nn.sigmoid(gate_preactivation)
    return squash * (1.0 + gate_preactivation * (1.0 - squash))


def slot_targets(route, cap):
    rows, top = route.shape
    flat = route.T.reshape(rows * top)
    before = jnp.arange(rows * top)[:, None] > jnp.arange(rows * top)[None, :]
    same = flat[:, None] == flat[None, :]
    ranks = jnp.sum((same & before).astype(jnp.int32), axis=1)
    return (flat * cap + ranks).reshape(top, rows)


RIGHT = [(i, (i + 1) % 4) for i in range(4)]
LEFT = [(i, (i - 1) % 4) for i in range(4)]


def first_hop(shard):
    return lax.ppermute(shard, "x", RIGHT), lax.ppermute(shard, "x", LEFT)


def second_hop(before, after):
    half = before.shape[0] // 2
    return lax.ppermute(before[:half], "x", RIGHT), lax.ppermute(after[half:], "x", LEFT)


def join_weights(where_ref, pieces, weight):
    x, zl = where_ref[0], where_ref[1]
    rows = weight.shape[0] // 8

    @pl.when(pl.program_id(0) == 0)
    def _():
        for n, piece in enumerate(pieces):
            line = zl if n < 4 else 1 - zl
            at = pl.multiple_of((line * 4 + (x + (0, 3, 1, 2)[n % 4]) % 4) * rows, rows)
            weight[pl.ds(at, rows), :] = piece[...]


def half_kernel(where_ref, x_ref, first_ref, *refs):
    frozen_ref, low_ref, weight = refs[8:]
    join_weights(where_ref, refs[:8], weight)
    frozen_ref[...] = dot(x_ref[...], weight[...])
    low_ref[...] = dot(x_ref[...], first_ref[...], ((1,), (1,)))


def final_kernel(where_ref, xa_ref, xb_ref, g_ref, frozen_ref, lowa_ref, first_ref, second_ref, *refs):
    out_ref, frozen_acc, slope_acc, sums, weight = refs[8:]
    join_weights(where_ref, refs[:8], weight)
    step = pl.program_id(0)
    low = (lowa_ref[...] + dot(xb_ref[...], first_ref[...], ((1,), (1,)))).astype(jnp.bfloat16)
    frozen_acc[...] = frozen_ref[...] + dot(xb_ref[...], weight[...])
    half = g_ref.shape[1] // 2
    for h in range(2):
        cols = slice(h * half, (h + 1) * half)
        preact = frozen_acc[:, cols] + ADAPTER_SCALE * dot(low, second_ref[:, cols])
        slope = g_ref[:, cols].astype(jnp.float32) * silu_slope(preact)
        slope_acc[:, cols] = slope.astype(jnp.bfloat16)
    back = dot(slope_acc[...], second_ref[...], ((1,), (1,))).astype(jnp.bfloat16)

    @pl.when(step == 0)
    def _():
        sums[...] = jnp.zeros_like(sums)

    width = xa_ref.shape[1] // 8
    for h, x_ref in enumerate((xa_ref, xb_ref)):
        part = dot(back, x_ref[...], ((0,), (0,)))
        for n in range(8):
            at = (2 * n + h) * width
            sums[:, at : at + width] += part[:, n * width : (n + 1) * width]
    sums[:, 16 * width :] += dot(low, slope_acc[...], ((0,), (0,)))

    @pl.when(step == pl.num_programs(0) - 1)
    def _():
        chunk = out_ref.shape[2]
        for n in range(4):
            out_ref[n] = ADAPTER_SCALE * sums[:, n * chunk : (n + 1) * chunk]


ROW_BLOCK = 256
EARLY = (4,)
LATE = (5, 3, 6, 7, 1)


def row_spec(array):
    return pl.BlockSpec((ROW_BLOCK, array.shape[1]), lambda i, w: (i, 0))


def whole_spec(array):
    return pl.BlockSpec(array.shape, lambda i, w: (0, 0))


def piece_specs(pieces, h):
    specs = []
    for piece in pieces:
        at = h if piece.shape[0] == 512 else 0
        specs.append(pl.BlockSpec((256, piece.shape[1]), lambda i, w, at=at: (at, 0)))
    return specs


def half_products(where, x, first, pieces, h):
    rows, hidden, rank = x.shape[0], pieces[0].shape[1], first.shape[0]
    return pl.pallas_call(
        half_kernel,
        grid_spec=pltpu.PrefetchScalarGridSpec(
            num_scalar_prefetch=1,
            grid=(rows // ROW_BLOCK,),
            in_specs=[row_spec(x), whole_spec(first)] + piece_specs(pieces, h),
            out_specs=[
                pl.BlockSpec((ROW_BLOCK, hidden), lambda i, w: (i, 0)),
                pl.BlockSpec((ROW_BLOCK, rank), lambda i, w: (i, 0)),
            ],
            scratch_shapes=[pltpu.VMEM((x.shape[1], hidden), jnp.bfloat16)],
        ),
        cost_estimate=pl.CostEstimate(
            flops=2 * rows * x.shape[1] * hidden, bytes_accessed=14 * 2**20, transcendentals=0
        ),
        out_shape=[
            jax.ShapeDtypeStruct((rows, hidden), jnp.float32),
            jax.ShapeDtypeStruct((rows, rank), jnp.float32),
        ],
        name="half_products",
    )(where, x, first, *pieces)


def gradients(where, xa, xb, g, frozen, low, first, second, pieces, h):
    rows, hidden, rank = xa.shape[0], pieces[0].shape[1], first.shape[0]
    total = 2 * xa.shape[1] + hidden
    by_row = [row_spec(v) for v in (xa, xb, g, frozen, low)]
    return pl.pallas_call(
        final_kernel,
        grid_spec=pltpu.PrefetchScalarGridSpec(
            num_scalar_prefetch=1,
            grid=(rows // ROW_BLOCK,),
            in_specs=by_row + [whole_spec(first), whole_spec(second)] + piece_specs(pieces, h),
            out_specs=pl.BlockSpec((4, rank, total // 4), lambda i, w: (0, 0, 0)),
            scratch_shapes=[
                pltpu.VMEM((ROW_BLOCK, hidden), jnp.float32),
                pltpu.VMEM((ROW_BLOCK, hidden), jnp.bfloat16),
                pltpu.VMEM((rank, total), jnp.float32),
                pltpu.VMEM((xa.shape[1], hidden), jnp.bfloat16),
            ],
        ),
        out_shape=jax.ShapeDtypeStruct((4, rank, total // 4), jnp.float32),
        name="gradients",
    )(where, xa, xb, g, frozen, low, first, second, *pieces)


def split_kernel(tokens_ref, *out_refs):
    for h, out_ref in enumerate(out_refs):
        for n in range(out_ref.shape[1] // 256):
            at = (2 * n + h) * 256
            out_ref[:, n * 256 : (n + 1) * 256] = tokens_ref[:, at : at + 256]


def split_columns(tokens):
    shape = jax.ShapeDtypeStruct((tokens.shape[0], tokens.shape[1] // 2), tokens.dtype)
    return pl.pallas_call(split_kernel, out_shape=[shape, shape], name="split_columns")(tokens)


def local(tokens, route, gate_output_gradient, frozen_gate_weight, adapter_first, adapter_second):
    tok_rows, width = tokens.shape
    hidden = gate_output_gradient.shape[2]
    cap = 12
    depth = 8
    zh, zl, x = lax.axis_index("zh"), lax.axis_index("zl"), lax.axis_index("x")
    half_width = width // 2

    lines = [
        lax.all_gather(part, ("zh", "zl"), axis=0, tiled=True) for part in split_columns(tokens)
    ]

    target = slot_targets(route, cap)
    line_target = jnp.broadcast_to(target[None], (depth, 2, tok_rows))
    line_target = lax.all_to_all(line_target, ("zh", "zl"), split_axis=0, concat_axis=0, tiled=True)

    mine = lax.dynamic_index_in_dim(frozen_gate_weight, zl, 0, keepdims=False)
    other = lax.dynamic_index_in_dim(frozen_gate_weight, 1 - zl, 0, keepdims=False)
    near = first_hop(mine)
    other, line_target = lax.optimization_barrier((other, line_target))
    got = lax.ppermute(other, "zl", [(0, 1), (1, 0)])

    row = jnp.arange(depth * depth * cap, dtype=jnp.int32)
    outer, inner, rank = row // (depth * cap), row // cap % depth, row % cap
    zi = zh * 2 + zl
    ahead = (zi + inner) % depth
    key = ((ahead // 2 * depth + outer) * 2 + ahead % 2) * cap + rank
    pick_g = key[:, None] == target.reshape(1, 2 * tok_rows)
    slots = jnp.concatenate([gate_output_gradient[:, k] for k in range(2)], axis=0)
    send_g = dot(pick_g.astype(jnp.bfloat16), slots).astype(jnp.bfloat16)
    send_g = send_g.reshape(depth, depth * cap, hidden)
    send_g, line_target = lax.optimization_barrier((send_g, line_target))
    column_g = lax.all_to_all(send_g, ("y", "c"), split_axis=0, concat_axis=0, tiled=True)
    swapped = (inner * depth + outer) * cap + rank
    swap = (swapped[:, None] == row[None, :]).astype(jnp.bfloat16)
    column_g = dot(swap, column_g.reshape(-1, hidden)).astype(jnp.bfloat16)

    line_target = line_target.transpose(1, 0, 2).reshape(2, depth * tok_rows)
    served = (zh * depth + outer) * 2 + zl
    key = (served * cap + row % cap)[:, None]
    col = jnp.arange(depth * tok_rows, dtype=jnp.int32)
    same_block = (row // cap % depth)[:, None] == (col // tok_rows)[None, :]
    pick = same_block & ((line_target[0][None] == key) | (line_target[1][None] == key))
    pick = pick.astype(jnp.bfloat16)

    def packed(line):
        return dot(pick, line).astype(jnp.bfloat16).reshape(depth, depth * cap, half_width)

    def spread(rows):
        rows = lax.all_to_all(rows, ("y", "c"), split_axis=0, concat_axis=0, tiled=True)
        return rows.reshape(depth * depth * cap, half_width)

    near_opposite = second_hop(*near)
    got, near_opposite, column_g = lax.optimization_barrier((got, near_opposite, column_g))
    far = first_hop(got)
    line0, near_opposite, column_g = lax.optimization_barrier((lines[0], near_opposite, column_g))
    xa = spread(packed(line0))
    blocks_g = [column_g[n * depth * cap : (n + 1) * depth * cap] for n in range(depth)]

    def pass_ahead(n):
        moves = [(i, (i + n) % depth) for i in range(depth)]
        return lax.ppermute(blocks_g[n], ("zh", "zl"), moves)

    two_ahead = pass_ahead(2)
    far_opposite = second_hop(*far)
    line1, far_opposite, blocks_g = lax.optimization_barrier((lines[1], far_opposite, blocks_g))
    for n in EARLY + LATE:
        blocks_g[n] = pass_ahead(n)
    blocks_g[2] = two_ahead
    xb = spread(packed(line1))

    behind = (zi - inner) % depth
    stand = jnp.where(behind < 3, behind, jnp.where(behind == 3, 7, jnp.where(behind == 4, 6, behind - 2)))
    order = (stand * depth + outer) * cap + rank
    order = (order[:, None] == row[None, :]).astype(jnp.bfloat16)
    rows_g = dot(order, jnp.concatenate([blocks_g[n] for n in (0, 1, 2, 5, 6, 7, 4, 3)], axis=0)).astype(jnp.bfloat16)

    first = lax.dynamic_index_in_dim(adapter_first, zl, 0, keepdims=False)
    second = lax.dynamic_index_in_dim(adapter_second, zl, 0, keepdims=False)
    first = first.T
    first_a, first_b = (
        jnp.concatenate([first[:, at : at + 256] for at in range(256 * h, width, 512)], axis=1)
        for h in range(2)
    )
    where = jnp.stack([x, zl]).astype(jnp.int32)
    pieces = [
        [mine, *near, near_opposite[h], got, *far, far_opposite[h]]
        for h in range(2)
    ]
    frozen, low = half_products(where, xa, first_a, pieces[0], 0)
    parts = gradients(where, xa, xb, rows_g, frozen, low, first_b, second, pieces[1], 1)

    rank, chunk = parts.shape[1:]
    parts = lax.all_to_all(parts, "x", split_axis=0, concat_axis=0, tiled=True)
    total = jnp.sum(parts, axis=0).astype(jnp.bfloat16)
    total = jnp.broadcast_to(total[None], (8, rank, chunk))
    total = lax.all_to_all(total, DP_AXES, split_axis=0, concat_axis=0, tiled=True)
    total = total.reshape(2, 4, rank, chunk).transpose(0, 2, 1, 3).reshape(2, rank, 4 * chunk)
    grad_a = total[:, :, :width].transpose(0, 2, 1).astype(jnp.float32)
    return grad_a, total[:, :, width:].astype(jnp.float32)


def solution(mesh):
    fine = Mesh(mesh.devices.reshape(4, 4, 2, 2, 4), EXPERT_AXES + DP_AXES)
    everyone = EXPERT_AXES + DP_AXES

    def step(*args):
        return local(*args)

    step = jax.shard_map(
        step,
        mesh=fine,
        in_specs=(
            P(everyone, None),
            P(everyone, None),
            P(everyone, None, None),
            P(EXPERT_AXES, DP_AXES, None),
            P(EXPERT_AXES, None, None),
            P(EXPERT_AXES, None, None),
        ),
        out_specs=(P(EXPERT_AXES, None, None), P(EXPERT_AXES, None, None)),
        check_vma=False,
    )
    return step
```
